32 devices in a mesh: gx: 4 (over z), gy: 8 (over y, x, core).
Axes of the slice: x: 2, y: 2, z: 4, core: 2. Of those that a mesh axis runs over, the one named last changes fastest.
Arguments:
- prolong: bfloat16 [2048, 24, 128], P(('gx', 'gy')), may hold values from -0.5 to 0.5
- stiffness: bfloat16 [4096, 4, 128, 128], P(('gx', 'gy')), may hold values from -6 to 6
- request: int32 [4096], P(('gx', 'gy')), may hold values from 0 to 63, as said below
- col_slot: int32 [4096, 4], P(('gx', 'gy')), may hold values from 0 to 127
- col_pos: int32 [4096, 4], P(('gx', 'gy')), may hold values from 0 to 15, as said below
- coarse_owner: int32 [2048, 1], P(('gx', 'gy')), may hold values from 0 to 31; in each aligned block of 64 rows (0 to 63, 64 to 127, ...) at most 4 rows name the same one
Outputs:
- coarse: float32 [4096, 24, 384], P(('gx', 'gy'))
The draws below stay inside these ranges and needn't reach their ends.
Inputs may be any that keep to these rules, and one draw needn't show every extreme that they name: `request`: on each device, entries k * 4 to (k + 1) * 4 - 1 name distinct aggregates of device k, as local indices there. `col_pos`: the 4 entries of one block row are distinct. `coarse_owner`: among one device's 64 aggregates at most 4 share a coarse owner, and on some devices 4 do.
All inputs are finite; a program needn't handle non-finite values.
Results may differ from the reference program's by a relative error of at most 0.0003.
Values may be sent and summed in bfloat16 or wider, within the bound.
A program may use at most 128 MiB of HBM per device.

```python
import math
import jax
import jax.numpy as jnp
import numpy as np
from jax import lax

AGG_DEV = 64
DOF = 128
CV = 24
MAXNB = 16
SLOT_DEV = 128
BPS = 4
SEND_MAX = 4
IN_ROWS = 128
NAGG = 2048
SLOTS = 4096
DEVICES = 32


def draw_request(key, part):
    per_peer = SLOT_DEV // DEVICES
    scores = jax.random.randint(key, (DEVICES * DEVICES, AGG_DEV), 0, 1 << 20) * AGG_DEV
    scores = scores + jnp.arange(AGG_DEV, dtype=jnp.int32)[None, :]
    chosen = jnp.argsort(scores, axis=1)[:, :per_peer]
    return chosen.reshape(-1).astype(jnp.int32)


def draw_col_pos(key, part):
    scores = jax.random.randint(key, (DEVICES * SLOT_DEV, MAXNB), 0, 1 << 20) * MAXNB
    scores = scores + jnp.arange(MAXNB, dtype=jnp.int32)[None, :]
    chosen = jnp.argsort(scores, axis=1)[:, :BPS]
    return chosen.astype(jnp.int32)


def touch_ends(values, key, low, high):
    longest = values.shape.index(max(values.shape))
    spots = []
    for shift in (0, 1):
        where = [jax.random.randint(jax.random.fold_in(key, axis), (), 0, length) for axis, length in enumerate(values.shape)]
        where[longest] = (where[longest] + shift) % values.shape[longest]
        spots.append(tuple(where))
    return values.at[spots[0]].set(low).at[spots[1]].set(high)


def level_of(own_key, shape, cuts, low, high):
    def one(position, shards_of):
        draws = jax.random.uniform(jax.random.fold_in(jax.random.fold_in(own_key, 6), position), (shards_of,), jnp.float32, low / len(cuts), high / len(cuts))
        return jnp.repeat(jnp.exp(draws), shape[position] // shards_of).reshape((-1,) + (1,) * (len(shape) - position - 1))

    factor_of = one(*cuts[0])
    for cut in cuts[1:]:
        factor_of = factor_of * one(*cut)
    return factor_of


def deal_out(stream_key, own, number, rows, count, top, reach, lean):
    order = jax.random.permutation(stream_key, count)
    heavy_load, common = load_shares(count, rows * top, reach, lean, True), load_shares(count, rows * top, reach, lean, False)
    places = jnp.arange(count)

    def named(sizes, offset_by):
        used = int((sizes > 0).sum())
        fixed = max(1, used // 4)
        shifted = fixed + (places - fixed + offset_by * (used - fixed)) % max(1, count - fixed)
        return jnp.zeros((count,), jnp.int32).at[order[jnp.where(places < fixed, places, shifted)]].set(jnp.asarray(sizes, jnp.int32))

    sizes = jnp.where(number % 4 == 0, named(heavy_load, number // 4), named(common, number - number // 4 - 1))
    mixed = jax.random.permutation(jax.random.fold_in(own, 3), count)
    source_of, taker = mixed[0:count // 2 * 2:2], mixed[1:count // 2 * 2:2]
    room = jnp.minimum(sizes[source_of] - 1, reach - sizes[taker]) // 2
    room = jnp.where((source_of == order[0]) | (taker == order[0]) | (sizes[taker] == 0), 0, jnp.maximum(room, 0))
    shifted = jax.random.randint(jax.random.fold_in(own, 4), (count // 2,), 0, 1 << 20) % (room + 1)
    sizes = sizes.at[source_of].add(-shifted).at[taker].add(shifted)
    items = jnp.searchsorted(jnp.cumsum(sizes), jnp.arange(rows * top), side="right").astype(jnp.int32)
    listing = items.reshape(top, rows).T
    listing = listing[jax.random.permutation(jax.random.fold_in(own, 1), rows)]
    offset_by = jax.random.randint(jax.random.fold_in(own, 2), (rows, 1), 0, top)
    return jnp.take_along_axis(listing, (jnp.arange(top)[None, :] + offset_by) % top, axis=1)


def load_shares(count, total, reach, slope, full):
    portions = [(1 << 20) // math.isqrt(rank ** slope) + 1 for rank in range(1, count + 1)]
    largest = reach if full else min(reach, max(-(-total // count), total * portions[0] // sum(portions)))
    least = 1 if total - largest >= count - 1 else 0
    holding, rest = [largest] + [least] * (count - 1), total - largest - least * (count - 1)
    while rest > 0:
        candidates = [i for i in range(1, count) if holding[i] < largest] or [i for i in range(1, count) if holding[i] < reach]
        whole, budget = sum([portions[i] for i in candidates]), rest
        for i in candidates:
            addition = min(reach - holding[i], max(1, budget * portions[i] // whole), rest)
            holding[i] = holding[i] + addition
            rest = rest - addition
    return np.array(holding)


def bell_draw(own_key, extent, width, limit, shards=(), held_as=jnp.bfloat16):
    values = width * jax.random.normal(own_key, extent, jnp.float32)
    if shards:
        values = values * level_of(own_key, extent, shards, -0.22, 0.18)
    return jnp.clip(values, -limit, limit).astype(held_as)


def setup_inputs(seed: int = 0) -> dict:
    arg_keys = jax.random.split(jax.random.key(seed), 7)
    prolong = bell_draw(arg_keys[0], (NAGG, CV, DOF), DOF ** -0.5, 0.5, ((0, 32),))
    stiffness = bell_draw(arg_keys[1], (SLOTS, BPS, DOF, DOF), 1.0, 6.0, ((0, 32),))
    request = draw_request(jax.random.fold_in(arg_keys[6], 71), 0)
    col_slot = touch_ends(jax.random.randint(arg_keys[3], (SLOTS, BPS), 0, SLOT_DEV), jax.random.fold_in(arg_keys[3], 1), 0, SLOT_DEV - 1).astype(jnp.int32)
    col_pos = draw_col_pos(jax.random.fold_in(arg_keys[6], 71), 0)
    coarse_owner_keys = jax.random.split(jax.random.fold_in(arg_keys[5], 1), NAGG // AGG_DEV)
    coarse_owner_turns = jax.random.permutation(jax.random.fold_in(arg_keys[5], 3), NAGG // AGG_DEV)
    coarse_owner = jax.vmap(lambda own, number: deal_out(jax.random.fold_in(arg_keys[5], 2), own, number, AGG_DEV, DEVICES, 1, SEND_MAX, 2))(coarse_owner_keys, coarse_owner_turns).reshape((NAGG, 1))
    return {"prolong": prolong, "stiffness": stiffness, "request": request, "col_slot": col_slot, "col_pos": col_pos, "coarse_owner": coarse_owner}


HIGH = lax.Precision.HIGHEST


def device_rows(prolong, stiff_block, request_block, slot_block, pos_block):
    per_peer = SLOT_DEV // DEVICES
    gid = (jnp.arange(SLOT_DEV, dtype=jnp.int32) // per_peer) * AGG_DEV + request_block.astype(jnp.int32)
    fetched = prolong[gid].astype(jnp.float32)
    col_rows = fetched[slot_block]
    applied = jnp.einsum("tqij,tqej->tqei", stiff_block.astype(jnp.float32), col_rows, precision=HIGH)
    partial_value = jnp.einsum("tci,tqei->tqce", fetched, applied, precision=HIGH)
    column_hot = (pos_block[:, :, None] == jnp.arange(MAXNB, dtype=jnp.int32)[None, None, :]).astype(jnp.float32)
    spread = jnp.einsum("tqce,tqn->tcne", partial_value, column_hot, precision=HIGH)
    return gid, spread.reshape(SLOT_DEV, CV, MAXNB * CV)


def reference(prolong, stiffness, request, col_slot, col_pos, coarse_owner):
    stiff_dev = stiffness.reshape(DEVICES, SLOT_DEV, BPS, DOF, DOF)
    request_dev = request.reshape(DEVICES, SLOT_DEV)
    slot_dev = col_slot.reshape(DEVICES, SLOT_DEV, BPS)
    pos_dev = col_pos.reshape(DEVICES, SLOT_DEV, BPS)

    def accumulate(total, pieces):
        gid, spread = device_rows(prolong, pieces[0], pieces[1], pieces[2], pieces[3])
        return total.at[gid].add(spread), None

    start = jnp.zeros((NAGG, CV, MAXNB * CV), jnp.float32)
    fine_coarse, _ = lax.scan(accumulate, start, (stiff_dev, request_dev, slot_dev, pos_dev))
    owners = coarse_owner[:, 0].reshape(DEVICES, AGG_DEV)
    peer_ids = jnp.arange(DEVICES, dtype=jnp.int32)
    owner_one = (owners[:, :, None] == peer_ids[None, None, :]).astype(jnp.int32)
    before = jnp.cumsum(owner_one, axis=1) - owner_one
    row_rank = jnp.sum(before * owner_one, axis=2)
    source = jnp.arange(DEVICES, dtype=jnp.int32)[:, None]
    target = (owners * IN_ROWS + source * SEND_MAX + row_rank).reshape(-1).astype(jnp.int32)
    coarse = jnp.zeros((DEVICES * IN_ROWS, CV, MAXNB * CV), jnp.float32).at[target].set(fine_coarse)
    return coarse
```

```python
import functools

import jax
import jax.numpy as jnp
from jax import lax
from jax.experimental import pallas as pl
from jax.experimental.pallas import tpu as pltpu
from jax.sharding import PartitionSpec as P

MAXNB = 16
AXES = ("gx", "gy")
LANES = 128
TOP = 32767.0
MESH = pl.DeviceIdType.MESH
HBM = pl.BlockSpec(memory_space=pl.ANY)
VMEM = pl.BlockSpec(memory_space=pltpu.VMEM)
SMEM = pl.BlockSpec(memory_space=pltpu.SMEM)
NT = (((1,), (1,)), ((), ()))


def exchange_kernel(gx, gy, count, *refs):
    ins, outs = refs[:count], refs[count : 2 * count]
    send_sem, recv_sem, local_sem = refs[2 * count :]
    n = gx * gy
    me = lax.axis_index("gx") * gy + lax.axis_index("gy")
    barrier = pltpu.get_barrier_semaphore()

    def greet(k, c):
        peer = lax.rem(me + k, n)
        pl.semaphore_signal(barrier, inc=1, device_id=(peer // gy, lax.rem(peer, gy)), device_id_type=MESH)
        return c

    lax.fori_loop(1, n, greet, 0)
    own = [pltpu.make_async_copy(ins[i].at[me], outs[i].at[me], local_sem.at[i]) for i in range(count)]
    for copy in own:
        copy.start()
    pl.semaphore_wait(barrier, n - 1)

    def copies(k, source):
        peer = lax.rem(me + k, n)
        return [
            pltpu.make_async_remote_copy(
                src_ref=ins[i].at[peer],
                dst_ref=outs[i].at[source],
                send_sem=send_sem.at[i, k],
                recv_sem=recv_sem.at[i, k],
                device_id=(peer // gy, lax.rem(peer, gy)),
                device_id_type=MESH,
            )
            for i in range(count)
        ]

    def send(k, c):
        for copy in copies(k, me):
            copy.start()
        return c

    lax.fori_loop(1, n, send, 0)

    def drain(k, c):
        for copy in copies(k, lax.rem(me + n - k, n)):
            copy.wait()
        return c

    lax.fori_loop(1, n, drain, 0)
    for copy in own:
        copy.wait()


def exchange(arrays, gx, gy, number):
    count = len(arrays)
    n = gx * gy
    return pl.pallas_call(
        functools.partial(exchange_kernel, gx, gy, count),
        out_shape=[jax.ShapeDtypeStruct(a.shape, a.dtype) for a in arrays],
        in_specs=[HBM] * count,
        out_specs=[HBM] * count,
        scratch_shapes=[
            pltpu.SemaphoreType.DMA((count, n)),
            pltpu.SemaphoreType.DMA((count, n)),
            pltpu.SemaphoreType.DMA((count,)),
        ],
        compiler_params=pltpu.CompilerParams(collective_id=number, has_side_effects=True),
        name=f"exchange{number}",
    )(*arrays)


def as_row(column):
    rows = column.shape[0]
    shape = (rows, LANES)
    eye = lax.broadcasted_iota(jnp.int32, shape, 0) == lax.broadcasted_iota(jnp.int32, shape, 1)
    return jnp.sum(jnp.where(eye, column, 0.0), axis=0, keepdims=True)


def as_column(row, rows):
    shape = (rows, LANES)
    eye = lax.broadcasted_iota(jnp.int32, shape, 0) == lax.broadcasted_iota(jnp.int32, shape, 1)
    return jnp.sum(jnp.where(eye, row, 0.0), axis=1, keepdims=True)


def coded(values):
    top = jnp.maximum(jnp.max(jnp.abs(values), axis=1, keepdims=True), 1e-30)
    code = jnp.round(values * (TOP / top)).astype(jnp.int32).astype(jnp.int16)
    return code, as_row(top * (1.0 / TOP))


def product_kernel(dims, slot_ref, fetched_ref, stiff_ref, *refs):
    cv, bps, group, per_step, quant = dims
    if quant:
        out_ref, scale_ref, wide_ref, cols_ref = refs
    else:
        out_ref, wide_ref, cols_ref = refs
    dof = stiff_ref.shape[-1]
    step = pl.program_id(0)
    span = bps * cv

    @pl.when(step == 0)
    def _():
        wide_ref[...] = fetched_ref[...].astype(jnp.float32)

    lane = lax.broadcasted_iota(jnp.int32, (dof, LANES), 1)

    def body(k, c):
        grp = step * per_step + k
        applied = []
        for tl in range(group):
            for q in range(bps):
                block = wide_ref[slot_ref[(grp * group + tl) * bps + q]]
                at = (span * tl + cv * q) % LANES
                first = min(cv, LANES - at)
                cols_ref[tl, at : at + first, :] = block[:first]
                if first < cv:
                    cols_ref[tl, 0 : cv - first, :] = block[first:]
            cols = cols_ref[tl].astype(jnp.bfloat16)
            mats = stiff_ref[k * group + tl].reshape(bps * dof, dof)
            prod = lax.dot_general(mats, cols, NT, preferred_element_type=jnp.float32)
            rel = (lane + (LANES * tl - span * tl) % LANES) % LANES
            one = prod[(bps - 1) * dof :]
            for q in range(bps - 2, -1, -1):
                one = jnp.where(rel < cv * (q + 1), prod[q * dof : (q + 1) * dof], one)
            applied.append(one)
        tiles = []
        for j in range(span * group // LANES):
            low, high = LANES * j // span, (LANES * (j + 1) - 1) // span
            tile = applied[high]
            for tl in range(high - 1, low - 1, -1):
                tile = jnp.where(lane < span * (tl + 1) - LANES * j, applied[tl], tile)
            tiles.append(tile)
        whole = jnp.concatenate(tiles, axis=1)
        hi = whole.astype(jnp.bfloat16)
        lo = (whole - hi.astype(jnp.float32)).astype(jnp.bfloat16)
        rows = wide_ref[pl.ds(grp * group, group)].reshape(group * cv, dof).astype(jnp.bfloat16)
        both = jnp.dot(rows, hi, preferred_element_type=jnp.float32) + jnp.dot(
            rows, lo, preferred_element_type=jnp.float32
        )
        wide_lane = lax.broadcasted_iota(jnp.int32, (cv, span * group), 1)
        out = both[(group - 1) * cv :]
        for tl in range(group - 2, -1, -1):
            out = jnp.where(wide_lane < span * (tl + 1), both[tl * cv : (tl + 1) * cv], out)
        if quant:
            out_ref[k], scale_ref[k] = coded(out)
        else:
            out_ref[k] = out
        return c

    lax.fori_loop(0, per_step, body, 0)


def products(fetched, stiffness, col_slot, group, quant):
    slots, cv, dof = fetched.shape
    bps = stiffness.shape[1]
    groups = slots // group
    per_step = 4 if groups % 4 == 0 else 1
    width = group * bps * cv
    out_shape = [jax.ShapeDtypeStruct((groups, cv, width), jnp.int16 if quant else jnp.float32)]
    out_specs = [pl.BlockSpec((per_step, cv, width), lambda i: (i, 0, 0))]
    if quant:
        out_shape.append(jax.ShapeDtypeStruct((groups, 1, LANES), jnp.float32))
        out_specs.append(pl.BlockSpec((per_step, 1, LANES), lambda i: (i, 0, 0)))
    return pl.pallas_call(
        functools.partial(product_kernel, (cv, bps, group, per_step, quant)),
        grid=(groups // per_step,),
        out_shape=out_shape,
        in_specs=[
            SMEM,
            pl.BlockSpec((slots, cv, dof), lambda i: (0, 0, 0)),
            pl.BlockSpec((per_step * group, bps, dof, dof), lambda i: (i, 0, 0, 0)),
        ],
        out_specs=out_specs,
        scratch_shapes=[
            pltpu.VMEM((slots, cv, dof), jnp.float32),
            pltpu.VMEM((group, LANES, dof), jnp.float32),
        ],
        compiler_params=pltpu.CompilerParams(vmem_limit_bytes=48 << 20),
        name="products",
    )(col_slot.reshape(-1), fetched, stiffness)


def gather_rows_kernel(dims, req_ref, owner_ref, target_ref, part_ref, *refs):
    cv, group, send_max, quant = dims
    if quant:
        scale_ref, out_ref, out_scale_ref, total_ref, place_ref, seen_ref = refs
    else:
        out_ref, out_scale_ref, total_ref, place_ref, seen_ref = refs
    n = out_ref.shape[0]
    groups, _, width = part_ref.shape
    span = width // group
    total_ref[...] = jnp.zeros_like(total_ref)

    def clear(i, c):
        seen_ref[i] = 0
        return c

    lax.fori_loop(0, n, clear, 0)

    def rank(a, c):
        owner = owner_ref[a]
        before = seen_ref[owner]
        place_ref[a] = owner * send_max + before
        seen_ref[owner] = before + 1
        return c

    lax.fori_loop(0, owner_ref.shape[0], rank, 0)
    lane = lax.broadcasted_iota(jnp.int32, (cv, width), 1)
    column = lax.broadcasted_iota(jnp.int32, (width, width), 0)

    def body(g, c):
        hot = jnp.where(column == target_ref[g], 1.0, 0.0).astype(jnp.bfloat16)
        if quant:
            code = part_ref[g].astype(jnp.int32)
            high = code >> 8
            pieces = [high.astype(jnp.float32), (code - high * 256).astype(jnp.float32)]
            weights = [256.0, 1.0]
        else:
            rest = part_ref[g]
            pieces, weights = [], [1.0, 1.0, 1.0]
            for _ in range(3):
                piece = rest.astype(jnp.bfloat16).astype(jnp.float32)
                pieces.append(piece)
                rest = rest - piece
        placed = 0.0
        for piece, weight in zip(pieces, weights):
            stack = jnp.concatenate(
                [
                    jnp.where((lane >= span * tl) & (lane < span * (tl + 1)), piece, 0.0)
                    for tl in range(group)
                ],
                axis=0,
            ).astype(jnp.bfloat16)
            placed = placed + weight * lax.dot_general(
                stack, hot, NT, preferred_element_type=jnp.float32
            )
        if quant:
            factor = as_column(scale_ref[g], cv)
        for tl in range(group):
            where = place_ref[req_ref[g * group + tl]]
            rows = placed[tl * cv : (tl + 1) * cv]
            if quant:
                rows = rows * factor
            total_ref[where] = total_ref[where] + rows
        return c

    lax.fori_loop(0, groups, body, 0)

    def emit(p, c):
        rows = total_ref[pl.ds(p * send_max, send_max)].reshape(send_max * cv, width)
        out_ref[p], out_scale_ref[p] = coded(rows)
        return c

    lax.fori_loop(0, n, emit, 0)


def gathered_rows(part, scale, target, requested, owners, n, send_max, group):
    groups, cv, width = part.shape
    quant = scale is not None
    args = [requested, owners, target, part] + ([scale] if quant else [])
    return pl.pallas_call(
        functools.partial(gather_rows_kernel, (cv, group, send_max, quant)),
        out_shape=[
            jax.ShapeDtypeStruct((n, send_max * cv, width), jnp.int16),
            jax.ShapeDtypeStruct((n, 1, LANES), jnp.float32),
        ],
        in_specs=[SMEM, SMEM] + [VMEM] * (len(args) - 2),
        out_specs=[VMEM, VMEM],
        scratch_shapes=[
            pltpu.VMEM((n * send_max, cv, width), jnp.float32),
            pltpu.SMEM((owners.shape[0],), jnp.int32),
            pltpu.SMEM((n,), jnp.int32),
        ],
        compiler_params=pltpu.CompilerParams(vmem_limit_bytes=48 << 20),
        name="gathered_rows",
    )(*args)


def decode_kernel(cv, code_ref, scale_ref, out_ref):
    per_step, rows, width = code_ref.shape

    for p in range(per_step):
        values = code_ref[p].astype(jnp.int32).astype(jnp.float32) * as_column(scale_ref[p], rows)
        out_ref[p * (rows // cv) : (p + 1) * (rows // cv)] = values.reshape(rows // cv, cv, width)


def decoded(code, scale, cv):
    n, rows, width = code.shape
    per_step = 4 if n % 4 == 0 else 1
    return pl.pallas_call(
        functools.partial(decode_kernel, cv),
        grid=(n // per_step,),
        out_shape=jax.ShapeDtypeStruct((n * rows // cv, cv, width), jnp.float32),
        in_specs=[
            pl.BlockSpec((per_step, rows, width), lambda i: (i, 0, 0)),
            pl.BlockSpec((per_step, 1, LANES), lambda i: (i, 0, 0)),
        ],
        out_specs=pl.BlockSpec((per_step * rows // cv, cv, width), lambda i: (i, 0, 0)),
        name="decoded",
    )(code, scale)


def per_device(gx, gy, prolong, stiffness, request, col_slot, col_pos, coarse_owner):
    n = gx * gy
    own_aggs, cv, dof = prolong.shape
    slots, bps = col_slot.shape
    per_peer = slots // n
    group = MAXNB // bps
    quant = per_peer == group
    send_max = (2 * own_aggs + n - 1) // n

    meta = jnp.concatenate([request.reshape(n, per_peer), col_pos.reshape(n, per_peer * bps)], axis=1)
    meta = jnp.pad(meta, ((0, 0), (0, LANES - meta.shape[1])))[:, None, :]
    (meta_in,) = exchange([meta], gx, gy, 1)
    requested = meta_in[:, 0, :per_peer].reshape(-1)
    pos_in = meta_in[:, 0, per_peer : per_peer * (1 + bps)].reshape(slots // group, group * bps)
    target = (cv * pos_in[:, :, None] + jnp.arange(cv, dtype=jnp.int32)).reshape(
        slots // group, 1, group * bps * cv
    )
    answer = prolong[requested].reshape(n, per_peer * cv, dof)
    (fetched,) = exchange([answer], gx, gy, 2)
    fetched = fetched.reshape(slots, cv, dof)
    made = products(fetched, stiffness, col_slot, group, quant)
    if quant:
        part, scale = exchange(made, gx, gy, 3)
    else:
        flat = made[0].reshape(slots // group, cv, group, bps * cv).transpose(0, 2, 1, 3)
        (flat,) = exchange([flat.reshape(n, per_peer * cv, bps * cv)], gx, gy, 3)
        flat = flat.reshape(slots // group, group, cv, bps * cv).transpose(0, 2, 1, 3)
        part, scale = flat.reshape(slots // group, cv, group * bps * cv), None
    code, factor = gathered_rows(
        part, scale, target, requested, coarse_owner[:, 0], n, send_max, group
    )
    code, factor = exchange([code, factor], gx, gy, 4)
    return decoded(code, factor, cv)


def solution(mesh):
    gx, gy = mesh.shape["gx"], mesh.shape["gy"]
    placed = (
        P(AXES, None, None),
        P(AXES, None, None, None),
        P(AXES),
        P(AXES, None),
        P(AXES, None),
        P(AXES, None),
    )
    return jax.shard_map(
        functools.partial(per_device, gx, gy),
        mesh=mesh,
        in_specs=placed,
        out_specs=P(AXES, None, None),
        check_vma=False,
    )
```

```python
import functools

import jax
import jax.numpy as jnp
from jax import lax
from jax.experimental import pallas as pl
from jax.experimental.pallas import tpu as pltpu
from jax.sharding import PartitionSpec as P

MAXNB = 16
AXES = ("gx", "gy")
LANES = 128
TOP = 32767.0
MESH = pl.DeviceIdType.MESH
HBM = pl.BlockSpec(memory_space=pl.ANY)
VMEM = pl.BlockSpec(memory_space=pltpu.VMEM)
SMEM = pl.BlockSpec(memory_space=pltpu.SMEM)
NT = (((1,), (1,)), ((), ()))


def exchange_kernel(gx, gy, count, *refs):
    ins, outs = refs[:count], refs[count : 2 * count]
    send_sem, recv_sem, local_sem = refs[2 * count :]
    n = gx * gy
    me = lax.axis_index("gx") * gy + lax.axis_index("gy")
    barrier = pltpu.get_barrier_semaphore()

    def greet(k, c):
        peer = lax.rem(me + k, n)
        pl.semaphore_signal(barrier, inc=1, device_id=(peer // gy, lax.rem(peer, gy)), device_id_type=MESH)
        return c

    lax.fori_loop(1, n, greet, 0)
    own = [pltpu.make_async_copy(ins[i].at[me], outs[i].at[me], local_sem.at[i]) for i in range(count)]
    for copy in own:
        copy.start()
    pl.semaphore_wait(barrier, n - 1)

    def copies(k, source):
        peer = lax.rem(me + k, n)
        return [
            pltpu.make_async_remote_copy(
                src_ref=ins[i].at[peer],
                dst_ref=outs[i].at[source],
                send_sem=send_sem.at[i, k],
                recv_sem=recv_sem.at[i, k],
                device_id=(peer // gy, lax.rem(peer, gy)),
                device_id_type=MESH,
            )
            for i in range(count)
        ]

    def send(k, c):
        for copy in copies(k, me):
            copy.start()
        return c

    lax.fori_loop(1, n, send, 0)

    def drain(k, c):
        for copy in copies(k, lax.rem(me + n - k, n)):
            copy.wait()
        return c

    lax.fori_loop(1, n, drain, 0)
    for copy in own:
        copy.wait()


def exchange(arrays, gx, gy, number):
    count = len(arrays)
    n = gx * gy
    return pl.pallas_call(
        functools.partial(exchange_kernel, gx, gy, count),
        out_shape=[jax.ShapeDtypeStruct(a.shape, a.dtype) for a in arrays],
        in_specs=[HBM] * count,
        out_specs=[HBM] * count,
        scratch_shapes=[
            pltpu.SemaphoreType.DMA((count, n)),
            pltpu.SemaphoreType.DMA((count, n)),
            pltpu.SemaphoreType.DMA((count,)),
        ],
        compiler_params=pltpu.CompilerParams(collective_id=number, has_side_effects=True),
        name=f"exchange{number}",
    )(*arrays)


def as_row(column):
    rows = column.shape[0]
    shape = (rows, LANES)
    eye = lax.broadcasted_iota(jnp.int32, shape, 0) == lax.broadcasted_iota(jnp.int32, shape, 1)
    return jnp.sum(jnp.where(eye, column, 0.0), axis=0, keepdims=True)


def as_column(row, rows):
    shape = (rows, LANES)
    eye = lax.broadcasted_iota(jnp.int32, shape, 0) == lax.broadcasted_iota(jnp.int32, shape, 1)
    return jnp.sum(jnp.where(eye, row, 0.0), axis=1, keepdims=True)


def coded(values):
    top = jnp.maximum(jnp.max(jnp.abs(values), axis=1, keepdims=True), 1e-30)
    code = jnp.round(values * (TOP / top)).astype(jnp.int32).astype(jnp.int16)
    return code, as_row(top * (1.0 / TOP))


def group_product(dims, grp, slot_ref, wide_ref, cols_ref, mats_of):
    cv, bps, group = dims
    dof = wide_ref.shape[-1]
    span = bps * cv
    lane = lax.broadcasted_iota(jnp.int32, (dof, LANES), 1)
    applied = []
    for tl in range(group):
        for q in range(bps):
            block = wide_ref[slot_ref[(grp * group + tl) * bps + q]]
            at = (span * tl + cv * q) % LANES
            first = min(cv, LANES - at)
            cols_ref[tl, at : at + first, :] = block[:first]
            if first < cv:
                cols_ref[tl, 0 : cv - first, :] = block[first:]
    for tl in range(group):
        cols = cols_ref[tl].astype(jnp.bfloat16)
        mats = mats_of(tl).reshape(bps * dof, dof)
        prod = lax.dot_general(mats, cols, NT, preferred_element_type=jnp.float32)
        rel = (lane + (LANES * tl - span * tl) % LANES) % LANES
        one = prod[(bps - 1) * dof :]
        for q in range(bps - 2, -1, -1):
            one = jnp.where(rel < cv * (q + 1), prod[q * dof : (q + 1) * dof], one)
        applied.append(one)
    tiles = []
    for j in range(span * group // LANES):
        low, high = LANES * j // span, (LANES * (j + 1) - 1) // span
        tile = applied[high]
        for tl in range(high - 1, low - 1, -1):
            tile = jnp.where(lane < span * (tl + 1) - LANES * j, applied[tl], tile)
        tiles.append(tile)
    whole = jnp.concatenate(tiles, axis=1)
    hi = whole.astype(jnp.bfloat16)
    lo = (whole - hi.astype(jnp.float32)).astype(jnp.bfloat16)
    rows = wide_ref[pl.ds(grp * group, group)].reshape(group * cv, dof).astype(jnp.bfloat16)
    both = jnp.dot(rows, hi, preferred_element_type=jnp.float32) + jnp.dot(
        rows, lo, preferred_element_type=jnp.float32
    )
    wide_lane = lax.broadcasted_iota(jnp.int32, (cv, span * group), 1)
    out = both[(group - 1) * cv :]
    for tl in range(group - 2, -1, -1):
        out = jnp.where(wide_lane < span * (tl + 1), both[tl * cv : (tl + 1) * cv], out)
    return out


def product_kernel(dims, slot_ref, fetched_ref, stiff_ref, out_ref, wide_ref, cols_ref):
    cv, bps, group, per_step = dims
    step = pl.program_id(0)

    @pl.when(step == 0)
    def _():
        wide_ref[...] = fetched_ref[...].astype(jnp.float32)

    def body(k, c):
        out_ref[k] = group_product(
            (cv, bps, group), step * per_step + k, slot_ref, wide_ref, cols_ref,
            lambda tl: stiff_ref[k * group + tl],
        )
        return c

    lax.fori_loop(0, per_step, body, 0)


def products(fetched, stiffness, col_slot, group):
    slots, cv, dof = fetched.shape
    bps = stiffness.shape[1]
    groups = slots // group
    per_step = 4 if groups % 4 == 0 else 1
    width = group * bps * cv
    return pl.pallas_call(
        functools.partial(product_kernel, (cv, bps, group, per_step)),
        grid=(groups // per_step,),
        out_shape=jax.ShapeDtypeStruct((groups, cv, width), jnp.float32),
        in_specs=[
            SMEM,
            pl.BlockSpec((slots, cv, dof), lambda i: (0, 0, 0)),
            pl.BlockSpec((per_step * group, bps, dof, dof), lambda i: (i, 0, 0, 0)),
        ],
        out_specs=pl.BlockSpec((per_step, cv, width), lambda i: (i, 0, 0)),
        scratch_shapes=[
            pltpu.VMEM((slots, cv, dof), jnp.float32),
            pltpu.VMEM((group, LANES, dof), jnp.float32),
        ],
        compiler_params=pltpu.CompilerParams(vmem_limit_bytes=48 << 20),
        name="products",
    )(col_slot.reshape(-1), fetched, stiffness)


def fused_kernel(
    dims,
    slot_ref, meta_ref, prolong_ref, stiff_ref,
    meta_out, part_out, scale_out,
    req_ref, stage_ref, fetched_ref, wide_ref, cols_ref, mats_ref, code_ref, factor_ref,
    meta_send, meta_recv, fetch_send, fetch_recv, part_send, part_recv, scale_send, scale_recv,
    mats_sem, own_sem,
):
    gx, gy, cv, bps, group = dims
    n = gx * gy
    me = lax.axis_index("gx") * gy + lax.axis_index("gy")
    barrier = pltpu.get_barrier_semaphore()

    def where(peer):
        return (peer // gy, lax.rem(peer, gy))

    def remote(src, dst, send_sem, recv_sem, peer):
        return pltpu.make_async_remote_copy(
            src_ref=src, dst_ref=dst, send_sem=send_sem, recv_sem=recv_sem,
            device_id=where(peer), device_id_type=MESH,
        )

    def meta_copy(k, peer, source):
        return remote(meta_ref.at[peer], meta_out.at[source], meta_send.at[k], meta_recv.at[k], peer)

    def fetch_copy(k, peer, source):
        return remote(
            stage_ref.at[pl.ds(peer * group, group)],
            fetched_ref.at[pl.ds(source * group, group)],
            fetch_send.at[k], fetch_recv.at[k], peer,
        )

    def part_copies(k, peer, source):
        return (
            remote(code_ref.at[peer], part_out.at[source], part_send.at[k], part_recv.at[k], peer),
            remote(factor_ref.at[peer], scale_out.at[source], scale_send.at[k], scale_recv.at[k], peer),
        )

    def mats_copy(peer):
        return pltpu.make_async_copy(
            stiff_ref.at[pl.ds(peer * group, group)],
            mats_ref.at[pl.ds(peer * group, group)],
            mats_sem.at[peer],
        )

    def greet(k, c):
        pl.semaphore_signal(barrier, inc=1, device_id=where(lax.rem(me + k, n)), device_id_type=MESH)
        return c

    lax.fori_loop(1, n, greet, 0)
    own_meta = pltpu.make_async_copy(meta_ref.at[me], meta_out.at[me], own_sem.at[0])
    own_meta.start()

    def load(k, c):
        mats_copy(lax.rem(me + k, n)).start()
        return c

    lax.fori_loop(1, n + 1, load, 0)
    pl.semaphore_wait(barrier, n - 1)

    def ask(k, c):
        meta_copy(k, lax.rem(me + k, n), me).start()
        return c

    lax.fori_loop(1, n, ask, 0)
    own_meta.wait()

    def asked(k, c):
        meta_copy(k, lax.rem(me + n - k, n), lax.rem(me + n - k, n)).wait()
        return c

    lax.fori_loop(1, n, asked, 0)
    to_scalars = pltpu.make_async_copy(meta_out, req_ref, own_sem.at[1])
    to_scalars.start()
    to_scalars.wait()

    def fill(k, c):
        peer = lax.rem(me + k, n)
        for j in range(group):
            stage_ref[peer * group + j] = prolong_ref[req_ref[peer, 0, j]]
        return c

    lax.fori_loop(1, n + 1, fill, 0)

    def answer(k, c):
        fetch_copy(k, lax.rem(me + k, n), me).start()
        return c

    lax.fori_loop(1, n, answer, 0)
    for j in range(group):
        wide_ref[me * group + j] = stage_ref[me * group + j].astype(jnp.float32)

    def take(k, c):
        source = lax.rem(me + n - k, n)
        fetch_copy(k, source, source).wait()
        for j in range(group):
            wide_ref[source * group + j] = fetched_ref[source * group + j].astype(jnp.float32)
        return c

    lax.fori_loop(1, n, take, 0)

    def work(k, c):
        peer = lax.rem(me + k, n)
        mats_copy(peer).wait()
        out = group_product(
            (cv, bps, group), peer, slot_ref, wide_ref, cols_ref,
            lambda tl: mats_ref[peer * group + tl],
        )
        code_ref[peer], factor_ref[peer] = coded(out)

        @pl.when(k > 1)
        def _():
            for copy in part_copies(k - 1, lax.rem(me + k - 1, n), me):
                copy.start()

        return c

    lax.fori_loop(1, n + 1, work, 0)
    own = (
        pltpu.make_async_copy(code_ref.at[me], part_out.at[me], own_sem.at[2]),
        pltpu.make_async_copy(factor_ref.at[me], scale_out.at[me], own_sem.at[3]),
    )
    for copy in own:
        copy.start()

    def drain(k, c):
        source = lax.rem(me + n - k, n)
        for copy in part_copies(k, source, source):
            copy.wait()
        return c

    lax.fori_loop(1, n, drain, 0)
    for copy in own:
        copy.wait()


def fused(meta, prolong, stiffness, col_slot, gx, gy, group):
    slots, bps, dof, _ = stiffness.shape
    cv = prolong.shape[1]
    n = gx * gy
    width = group * bps * cv
    sem = pltpu.SemaphoreType.DMA
    return pl.pallas_call(
        functools.partial(fused_kernel, (gx, gy, cv, bps, group)),
        out_shape=[
            jax.ShapeDtypeStruct(meta.shape, jnp.int32),
            jax.ShapeDtypeStruct((n, cv, width), jnp.int16),
            jax.ShapeDtypeStruct((n, 1, LANES), jnp.float32),
        ],
        in_specs=[SMEM, VMEM, VMEM, HBM],
        out_specs=[VMEM, VMEM, VMEM],
        scratch_shapes=[
            pltpu.SMEM(meta.shape, jnp.int32),
            pltpu.VMEM((slots, cv, dof), jnp.bfloat16),
            pltpu.VMEM((slots, cv, dof), jnp.bfloat16),
            pltpu.VMEM((slots, cv, dof), jnp.float32),
            pltpu.VMEM((group, LANES, dof), jnp.float32),
            pltpu.VMEM((slots, bps, dof, dof), jnp.bfloat16),
            pltpu.VMEM((n, cv, width), jnp.int16),
            pltpu.VMEM((n, 1, LANES), jnp.float32),
        ]
        + [sem((n,))] * 9
        + [sem((4,))],
        compiler_params=pltpu.CompilerParams(
            collective_id=1, has_side_effects=True, vmem_limit_bytes=56 << 20
        ),
        name="fused",
    )(col_slot.reshape(-1), meta, prolong, stiffness)


def gather_rows_kernel(dims, meta_ref, owner_ref, part_ref, *refs):
    cv, bps, per_peer, group, send_max, quant = dims
    if quant:
        scale_ref, out_ref, out_scale_ref, total_ref, place_ref, seen_ref = refs
    else:
        out_ref, out_scale_ref, total_ref, place_ref, seen_ref = refs
    n = out_ref.shape[0]
    groups, _, width = part_ref.shape
    span = width // group
    total_ref[...] = jnp.zeros_like(total_ref)

    def clear(i, c):
        seen_ref[i] = 0
        return c

    lax.fori_loop(0, n, clear, 0)

    def rank(a, c):
        owner = owner_ref[a]
        before = seen_ref[owner]
        place_ref[a] = owner * send_max + before
        seen_ref[owner] = before + 1
        return c

    lax.fori_loop(0, owner_ref.shape[0], rank, 0)
    lane = lax.broadcasted_iota(jnp.int32, (cv, width), 1)
    column = lax.broadcasted_iota(jnp.int32, (width, width), 0)
    row_lane = lax.broadcasted_iota(jnp.int32, (1, width), 1)

    def body(g, c):
        at = row_lane
        for j in range(group * bps):
            t = g * group + j // bps
            pos = meta_ref[t // per_peer, 0, per_peer + (t % per_peer) * bps + j % bps]
            at = at + jnp.where(row_lane // cv == j, cv * (pos - j), 0)
        hot = jnp.where(column == at, 1.0, 0.0).astype(jnp.bfloat16)
        if quant:
            code = part_ref[g].astype(jnp.int32)
            high = code >> 8
            pieces = [high.astype(jnp.float32), (code - high * 256).astype(jnp.float32)]
            weights = [256.0, 1.0]
        else:
            rest = part_ref[g]
            pieces, weights = [], [1.0, 1.0, 1.0]
            for _ in range(3):
                piece = rest.astype(jnp.bfloat16).astype(jnp.float32)
                pieces.append(piece)
                rest = rest - piece
        placed = 0.0
        for piece, weight in zip(pieces, weights):
            stack = jnp.concatenate(
                [
                    jnp.where((lane >= span * tl) & (lane < span * (tl + 1)), piece, 0.0)
                    for tl in range(group)
                ],
                axis=0,
            ).astype(jnp.bfloat16)
            placed = placed + weight * lax.dot_general(
                stack, hot, NT, preferred_element_type=jnp.float32
            )
        if quant:
            factor = as_column(scale_ref[g], cv)
        for tl in range(group):
            t = g * group + tl
            where = place_ref[meta_ref[t // per_peer, 0, t % per_peer]]
            rows = placed[tl * cv : (tl + 1) * cv]
            if quant:
                rows = rows * factor
            total_ref[where] = total_ref[where] + rows
        return c

    lax.fori_loop(0, groups, body, 0)

    def emit(p, c):
        rows = total_ref[pl.ds(p * send_max, send_max)].reshape(send_max * cv, width)
        out_ref[p], out_scale_ref[p] = coded(rows)
        return c

    lax.fori_loop(0, n, emit, 0)


def gathered_rows(part, scale, meta, owners, n, send_max, group, bps, per_peer):
    groups, cv, width = part.shape
    quant = scale is not None
    args = [meta, owners, part] + ([scale] if quant else [])
    return pl.pallas_call(
        functools.partial(gather_rows_kernel, (cv, bps, per_peer, group, send_max, quant)),
        out_shape=[
            jax.ShapeDtypeStruct((n, send_max * cv, width), jnp.int16),
            jax.ShapeDtypeStruct((n, 1, LANES), jnp.float32),
        ],
        in_specs=[SMEM, SMEM] + [VMEM] * (len(args) - 2),
        out_specs=[VMEM, VMEM],
        scratch_shapes=[
            pltpu.VMEM((n * send_max, cv, width), jnp.float32),
            pltpu.SMEM((owners.shape[0],), jnp.int32),
            pltpu.SMEM((n,), jnp.int32),
        ],
        compiler_params=pltpu.CompilerParams(vmem_limit_bytes=48 << 20),
        name="gathered_rows",
    )(*args)


def decode_kernel(cv, code_ref, scale_ref, out_ref):
    per_step, rows, width = code_ref.shape

    for p in range(per_step):
        values = code_ref[p].astype(jnp.int32).astype(jnp.float32) * as_column(scale_ref[p], rows)
        out_ref[p * (rows // cv) : (p + 1) * (rows // cv)] = values.reshape(rows // cv, cv, width)


def decoded(code, scale, cv):
    n, rows, width = code.shape
    per_step = 4 if n % 4 == 0 else 1
    return pl.pallas_call(
        functools.partial(decode_kernel, cv),
        grid=(n // per_step,),
        out_shape=jax.ShapeDtypeStruct((n * rows // cv, cv, width), jnp.float32),
        in_specs=[
            pl.BlockSpec((per_step, rows, width), lambda i: (i, 0, 0)),
            pl.BlockSpec((per_step, 1, LANES), lambda i: (i, 0, 0)),
        ],
        out_specs=pl.BlockSpec((per_step * rows // cv, cv, width), lambda i: (i, 0, 0)),
        name="decoded",
    )(code, scale)


def per_device(gx, gy, prolong, stiffness, request, col_slot, col_pos, coarse_owner):
    n = gx * gy
    own_aggs, cv, dof = prolong.shape
    slots, bps = col_slot.shape
    per_peer = slots // n
    group = MAXNB // bps
    quant = per_peer == group
    send_max = (2 * own_aggs + n - 1) // n

    meta = jnp.concatenate([request.reshape(n, per_peer), col_pos.reshape(n, per_peer * bps)], axis=1)
    meta = jnp.pad(meta, ((0, 0), (0, LANES - meta.shape[1])))[:, None, :]
    if quant:
        meta_in, part, scale = fused(meta, prolong, stiffness, col_slot, gx, gy, group)
    else:
        (meta_in,) = exchange([meta], gx, gy, 1)
        answer = prolong[meta_in[:, 0, :per_peer].reshape(-1)].reshape(n, per_peer * cv, dof)
        (fetched,) = exchange([answer], gx, gy, 2)
        made = products(fetched.reshape(slots, cv, dof), stiffness, col_slot, group)
        flat = made.reshape(slots // group, cv, group, bps * cv).transpose(0, 2, 1, 3)
        (flat,) = exchange([flat.reshape(n, per_peer * cv, bps * cv)], gx, gy, 3)
        flat = flat.reshape(slots // group, group, cv, bps * cv).transpose(0, 2, 1, 3)
        part, scale = flat.reshape(slots // group, cv, group * bps * cv), None
    code, factor = gathered_rows(
        part, scale, meta_in, coarse_owner[:, 0], n, send_max, group, bps, per_peer
    )
    code, factor = exchange([code, factor], gx, gy, 4)
    return decoded(code, factor, cv)


def solution(mesh):
    gx, gy = mesh.shape["gx"], mesh.shape["gy"]
    placed = (
        P(AXES, None, None),
        P(AXES, None, None, None),
        P(AXES),
        P(AXES, None),
        P(AXES, None),
        P(AXES, None),
    )
    return jax.shard_map(
        functools.partial(per_device, gx, gy),
        mesh=mesh,
        in_specs=placed,
        out_specs=P(AXES, None, None),
        check_vma=False,
    )
```

```python
import functools

import jax
import jax.numpy as jnp
from jax import lax
from jax.experimental import pallas as pl
from jax.experimental.pallas import tpu as pltpu
from jax.sharding import PartitionSpec as P

MAXNB = 16
AXES = ("gx", "gy")
LANES = 128
TOP = 32767.0
MESH = pl.DeviceIdType.MESH
HBM = pl.BlockSpec(memory_space=pl.ANY)
VMEM = pl.BlockSpec(memory_space=pltpu.VMEM)
SMEM = pl.BlockSpec(memory_space=pltpu.SMEM)
NT = (((1,), (1,)), ((), ()))


def peer_at(k, gx, gy, mixed):
    n = gx * gy
    x, y = lax.axis_index("gx"), lax.axis_index("gy")
    if gx % 2:
        return lax.rem(x * gy + y + 1 + k, n)
    half = gx // 2
    count = half * gy
    if mixed:
        near, i = lax.rem(k, 2), k // 2
    else:
        near, i = k // count, lax.rem(k, count)
    i = lax.rem(i + near, count)
    side = lax.rem(x // half + 1 + near, 2)
    row = side * half + lax.rem(x + i // gy, half)
    return row * gy + lax.rem(y + i, gy)


def deliver_kernel(dims, code_ref, scale_ref, out_ref, land_ref, land_scale, wide_ref, *sems):
    gx, gy, cv = dims
    code_send, code_recv, scale_send, scale_recv, out_sem = sems
    n, rows, width = code_ref.shape
    take = rows // cv
    me = lax.axis_index("gx") * gy + lax.axis_index("gy")
    barrier = pltpu.get_barrier_semaphore()

    def where(peer):
        return (peer // gy, lax.rem(peer, gy))

    def greet(k, c):
        peer = peer_at(k, gx, gy, True)
        pl.semaphore_signal(barrier, inc=1, device_id=where(peer), device_id_type=MESH)
        return c

    lax.fori_loop(0, n - 1, greet, 0)

    def copies(peer, source):
        return [
            pltpu.make_async_remote_copy(
                src_ref=src.at[peer], dst_ref=dst.at[source],
                send_sem=send.at[peer], recv_sem=recv.at[source],
                device_id=where(peer), device_id_type=MESH,
            )
            for src, dst, send, recv in (
                (scale_ref, land_scale, scale_send, scale_recv),
                (code_ref, land_ref, code_send, code_recv),
            )
        ]

    def out_copy(p):
        at = pl.ds(p * take, take)
        return pltpu.make_async_copy(wide_ref.at[at], out_ref.at[at], out_sem.at[p])

    pl.semaphore_wait(barrier, n - 1)

    def send(k, c):
        for copy in copies(peer_at(k, gx, gy, True), me):
            copy.start()
        return c

    lax.fori_loop(0, n - 1, send, 0)

    def decode(code, scale, p):
        values = code.astype(jnp.int32).astype(jnp.float32) * as_column(scale, rows)
        wide_ref[pl.ds(p * take, take)] = values.reshape(take, cv, width)
        out_copy(p).start()

    decode(code_ref[me], scale_ref[me], me)

    def drain(k, c):
        source = peer_at(k, gx, gy, True)
        for copy in copies(source, source):
            copy.wait()
        decode(land_ref[source], land_scale[source], source)
        return c

    lax.fori_loop(0, n - 1, drain, 0)

    def finish(p, c):
        out_copy(p).wait()
        return c

    lax.fori_loop(0, n, finish, 0)


def delivered(code, scale, cv, gx, gy):
    n, rows, width = code.shape
    sem = pltpu.SemaphoreType.DMA
    out = (n * rows // cv, cv, width)
    return pl.pallas_call(
        functools.partial(deliver_kernel, (gx, gy, cv)),
        out_shape=jax.ShapeDtypeStruct(out, jnp.float32),
        in_specs=[VMEM, VMEM],
        out_specs=HBM,
        scratch_shapes=[
            pltpu.VMEM(code.shape, jnp.int16),
            pltpu.VMEM(scale.shape, jnp.float32),
            pltpu.VMEM(out, jnp.float32),
        ]
        + [sem((n,))] * 5,
        compiler_params=pltpu.CompilerParams(
            collective_id=4, has_side_effects=True, vmem_limit_bytes=40 << 20
        ),
        name="delivered",
    )(code, scale)


def exchange_kernel(gx, gy, count, *refs):
    ins, outs = refs[:count], refs[count : 2 * count]
    send_sem, recv_sem, local_sem = refs[2 * count :]
    n = gx * gy
    me = lax.axis_index("gx") * gy + lax.axis_index("gy")
    barrier = pltpu.get_barrier_semaphore()

    def greet(k, c):
        peer = lax.rem(me + k, n)
        pl.semaphore_signal(barrier, inc=1, device_id=(peer // gy, lax.rem(peer, gy)), device_id_type=MESH)
        return c

    lax.fori_loop(1, n, greet, 0)
    own = [pltpu.make_async_copy(ins[i].at[me], outs[i].at[me], local_sem.at[i]) for i in range(count)]
    for copy in own:
        copy.start()
    pl.semaphore_wait(barrier, n - 1)

    def copies(k, source):
        peer = lax.rem(me + k, n)
        return [
            pltpu.make_async_remote_copy(
                src_ref=ins[i].at[peer],
                dst_ref=outs[i].at[source],
                send_sem=send_sem.at[i, k],
                recv_sem=recv_sem.at[i, k],
                device_id=(peer // gy, lax.rem(peer, gy)),
                device_id_type=MESH,
            )
            for i in range(count)
        ]

    def send(k, c):
        for copy in copies(k, me):
            copy.start()
        return c

    lax.fori_loop(1, n, send, 0)

    def drain(k, c):
        for copy in copies(k, lax.rem(me + n - k, n)):
            copy.wait()
        return c

    lax.fori_loop(1, n, drain, 0)
    for copy in own:
        copy.wait()


def exchange(arrays, gx, gy, number):
    count = len(arrays)
    n = gx * gy
    return pl.pallas_call(
        functools.partial(exchange_kernel, gx, gy, count),
        out_shape=[jax.ShapeDtypeStruct(a.shape, a.dtype) for a in arrays],
        in_specs=[HBM] * count,
        out_specs=[HBM] * count,
        scratch_shapes=[
            pltpu.SemaphoreType.DMA((count, n)),
            pltpu.SemaphoreType.DMA((count, n)),
            pltpu.SemaphoreType.DMA((count,)),
        ],
        compiler_params=pltpu.CompilerParams(collective_id=number, has_side_effects=True),
        name=f"exchange{number}",
    )(*arrays)


def as_row(column):
    rows = column.shape[0]
    shape = (rows, LANES)
    eye = lax.broadcasted_iota(jnp.int32, shape, 0) == lax.broadcasted_iota(jnp.int32, shape, 1)
    return jnp.sum(jnp.where(eye, column, 0.0), axis=0, keepdims=True)


def as_column(row, rows):
    shape = (rows, LANES)
    eye = lax.broadcasted_iota(jnp.int32, shape, 0) == lax.broadcasted_iota(jnp.int32, shape, 1)
    return jnp.sum(jnp.where(eye, row, 0.0), axis=1, keepdims=True)


def coded(values):
    top = jnp.maximum(jnp.max(jnp.abs(values), axis=1, keepdims=True), 1e-30)
    code = jnp.round(values * (TOP / top)).astype(jnp.int32).astype(jnp.int16)
    return code, as_row(top * (1.0 / TOP))


def group_product(dims, grp, slot_ref, wide_ref, cols_ref, mats_of):
    cv, bps, group = dims
    dof = wide_ref.shape[-1]
    span = bps * cv
    lane = lax.broadcasted_iota(jnp.int32, (dof, LANES), 1)
    applied = []
    for tl in range(group):
        for q in range(bps):
            block = wide_ref[slot_ref[(grp * group + tl) * bps + q]]
            at = (span * tl + cv * q) % LANES
            first = min(cv, LANES - at)
            cols_ref[tl, at : at + first, :] = block[:first]
            if first < cv:
                cols_ref[tl, 0 : cv - first, :] = block[first:]
    for tl in range(group):
        cols = cols_ref[tl].astype(jnp.bfloat16)
        mats = mats_of(tl).reshape(bps * dof, dof)
        prod = lax.dot_general(mats, cols, NT, preferred_element_type=jnp.float32)
        rel = (lane + (LANES * tl - span * tl) % LANES) % LANES
        one = prod[(bps - 1) * dof :]
        for q in range(bps - 2, -1, -1):
            one = jnp.where(rel < cv * (q + 1), prod[q * dof : (q + 1) * dof], one)
        applied.append(one)
    tiles = []
    for j in range(span * group // LANES):
        low, high = LANES * j // span, (LANES * (j + 1) - 1) // span
        tile = applied[high]
        for tl in range(high - 1, low - 1, -1):
            tile = jnp.where(lane < span * (tl + 1) - LANES * j, applied[tl], tile)
        tiles.append(tile)
    whole = jnp.concatenate(tiles, axis=1)
    hi = whole.astype(jnp.bfloat16)
    lo = (whole - hi.astype(jnp.float32)).astype(jnp.bfloat16)
    rows = wide_ref[pl.ds(grp * group, group)].reshape(group * cv, dof).astype(jnp.bfloat16)
    both = jnp.dot(rows, hi, preferred_element_type=jnp.float32) + jnp.dot(
        rows, lo, preferred_element_type=jnp.float32
    )
    wide_lane = lax.broadcasted_iota(jnp.int32, (cv, span * group), 1)
    out = both[(group - 1) * cv :]
    for tl in range(group - 2, -1, -1):
        out = jnp.where(wide_lane < span * (tl + 1), both[tl * cv : (tl + 1) * cv], out)
    return out


def product_kernel(dims, slot_ref, fetched_ref, stiff_ref, out_ref, wide_ref, cols_ref):
    cv, bps, group, per_step = dims
    step = pl.program_id(0)

    @pl.when(step == 0)
    def _():
        wide_ref[...] = fetched_ref[...].astype(jnp.float32)

    def body(k, c):
        out_ref[k] = group_product(
            (cv, bps, group), step * per_step + k, slot_ref, wide_ref, cols_ref,
            lambda tl: stiff_ref[k * group + tl],
        )
        return c

    lax.fori_loop(0, per_step, body, 0)


def products(fetched, stiffness, col_slot, group):
    slots, cv, dof = fetched.shape
    bps = stiffness.shape[1]
    groups = slots // group
    per_step = 4 if groups % 4 == 0 else 1
    width = group * bps * cv
    return pl.pallas_call(
        functools.partial(product_kernel, (cv, bps, group, per_step)),
        grid=(groups // per_step,),
        out_shape=jax.ShapeDtypeStruct((groups, cv, width), jnp.float32),
        in_specs=[
            SMEM,
            pl.BlockSpec((slots, cv, dof), lambda i: (0, 0, 0)),
            pl.BlockSpec((per_step * group, bps, dof, dof), lambda i: (i, 0, 0, 0)),
        ],
        out_specs=pl.BlockSpec((per_step, cv, width), lambda i: (i, 0, 0)),
        scratch_shapes=[
            pltpu.VMEM((slots, cv, dof), jnp.float32),
            pltpu.VMEM((group, LANES, dof), jnp.float32),
        ],
        compiler_params=pltpu.CompilerParams(vmem_limit_bytes=48 << 20),
        name="products",
    )(col_slot.reshape(-1), fetched, stiffness)


def fused_kernel(
    dims,
    slot_ref, meta_ref, prolong_ref, stiff_ref,
    meta_out, part_out, scale_out,
    req_ref, stage_ref, fetched_ref, wide_ref, cols_ref, mats_ref, code_ref, factor_ref,
    meta_send, meta_recv, fetch_send, fetch_recv, part_send, part_recv, scale_send, scale_recv,
    mats_sem, own_sem,
):
    gx, gy, cv, bps, group = dims
    n = gx * gy
    me = lax.axis_index("gx") * gy + lax.axis_index("gy")
    barrier = pltpu.get_barrier_semaphore()

    def where(peer):
        return (peer // gy, lax.rem(peer, gy))

    def remote(src, dst, send_sem, recv_sem, peer):
        return pltpu.make_async_remote_copy(
            src_ref=src, dst_ref=dst, send_sem=send_sem, recv_sem=recv_sem,
            device_id=where(peer), device_id_type=MESH,
        )

    def meta_copy(peer, source):
        return remote(
            meta_ref.at[peer], meta_out.at[source], meta_send.at[peer], meta_recv.at[source], peer
        )

    def fetch_copy(peer, source):
        return remote(
            stage_ref.at[pl.ds(peer * group, group)],
            fetched_ref.at[pl.ds(source * group, group)],
            fetch_send.at[peer], fetch_recv.at[source], peer,
        )

    def part_copies(peer, source):
        return (
            remote(code_ref.at[peer], part_out.at[source], part_send.at[peer], part_recv.at[source], peer),
            remote(
                factor_ref.at[peer], scale_out.at[source], scale_send.at[peer], scale_recv.at[source], peer
            ),
        )

    def mats_copy(peer):
        return pltpu.make_async_copy(
            stiff_ref.at[pl.ds(peer * group, group)],
            mats_ref.at[pl.ds(peer * group, group)],
            mats_sem.at[peer],
        )

    def greet(k, c):
        pl.semaphore_signal(barrier, inc=1, device_id=where(lax.rem(me + k, n)), device_id_type=MESH)
        return c

    lax.fori_loop(1, n, greet, 0)
    own_meta = pltpu.make_async_copy(meta_ref.at[me], meta_out.at[me], own_sem.at[0])
    own_meta.start()

    def load(k, c):
        mats_copy(peer_at(k, gx, gy, False)).start()
        return c

    lax.fori_loop(0, n, load, 0)
    pl.semaphore_wait(barrier, n - 1)

    def ask(k, c):
        meta_copy(peer_at(k, gx, gy, True), me).start()
        return c

    lax.fori_loop(0, n - 1, ask, 0)
    own_meta.wait()

    def asked(k, c):
        source = peer_at(k, gx, gy, True)
        meta_copy(source, source).wait()
        return c

    lax.fori_loop(0, n - 1, asked, 0)
    to_scalars = pltpu.make_async_copy(meta_out, req_ref, own_sem.at[1])
    to_scalars.start()
    to_scalars.wait()

    def fill(k, c):
        peer = peer_at(k, gx, gy, True)
        for j in range(group):
            stage_ref[peer * group + j] = prolong_ref[req_ref[peer, 0, j]]
        return c

    lax.fori_loop(0, n, fill, 0)

    def answer(k, c):
        fetch_copy(peer_at(k, gx, gy, True), me).start()
        return c

    lax.fori_loop(0, n - 1, answer, 0)
    for j in range(group):
        wide_ref[me * group + j] = stage_ref[me * group + j].astype(jnp.float32)

    def take(k, c):
        source = peer_at(k, gx, gy, True)
        fetch_copy(source, source).wait()
        for j in range(group):
            wide_ref[source * group + j] = fetched_ref[source * group + j].astype(jnp.float32)
        return c

    lax.fori_loop(0, n - 1, take, 0)
    wide_step = 2 if n % 2 == 0 else 1

    def work(i, c):
        for u in range(wide_step):
            mats_copy(peer_at(i * wide_step + u, gx, gy, False)).wait()
        for u in range(wide_step):
            peer = peer_at(i * wide_step + u, gx, gy, False)
            out = group_product(
                (cv, bps, group), peer, slot_ref, wide_ref, cols_ref.at[u],
                lambda tl: mats_ref[peer * group + tl],
            )
            code_ref[peer], factor_ref[peer] = coded(out)

        @pl.when(i > 0)
        def _():
            for u in range(wide_step):
                for copy in part_copies(peer_at((i - 1) * wide_step + u, gx, gy, False), me):
                    copy.start()

        return c

    lax.fori_loop(0, n // wide_step, work, 0)
    for k in range(n - wide_step, n - 1):
        for copy in part_copies(peer_at(k, gx, gy, False), me):
            copy.start()
    own = (
        pltpu.make_async_copy(code_ref.at[me], part_out.at[me], own_sem.at[2]),
        pltpu.make_async_copy(factor_ref.at[me], scale_out.at[me], own_sem.at[3]),
    )
    for copy in own:
        copy.start()

    def drain(k, c):
        source = peer_at(k, gx, gy, False)
        for copy in part_copies(source, source):
            copy.wait()
        return c

    lax.fori_loop(0, n - 1, drain, 0)
    for copy in own:
        copy.wait()


def fused(meta, prolong, stiffness, col_slot, gx, gy, group):
    slots, bps, dof, _ = stiffness.shape
    cv = prolong.shape[1]
    n = gx * gy
    width = group * bps * cv
    sem = pltpu.SemaphoreType.DMA
    return pl.pallas_call(
        functools.partial(fused_kernel, (gx, gy, cv, bps, group)),
        out_shape=[
            jax.ShapeDtypeStruct(meta.shape, jnp.int32),
            jax.ShapeDtypeStruct((n, cv, width), jnp.int16),
            jax.ShapeDtypeStruct((n, 1, LANES), jnp.float32),
        ],
        in_specs=[SMEM, VMEM, VMEM, HBM],
        out_specs=[VMEM, VMEM, VMEM],
        scratch_shapes=[
            pltpu.SMEM(meta.shape, jnp.int32),
            pltpu.VMEM((slots, cv, dof), jnp.bfloat16),
            pltpu.VMEM((slots, cv, dof), jnp.bfloat16),
            pltpu.VMEM((slots, cv, dof), jnp.float32),
            pltpu.VMEM((2, group, LANES, dof), jnp.float32),
            pltpu.VMEM((slots, bps, dof, dof), jnp.bfloat16),
            pltpu.VMEM((n, cv, width), jnp.int16),
            pltpu.VMEM((n, 1, LANES), jnp.float32),
        ]
        + [sem((n,))] * 9
        + [sem((4,))],
        compiler_params=pltpu.CompilerParams(
            collective_id=1, has_side_effects=True, vmem_limit_bytes=56 << 20
        ),
        name="fused",
    )(col_slot.reshape(-1), meta, prolong, stiffness)


def gather_rows_kernel(dims, meta_ref, owner_ref, part_ref, *refs):
    cv, bps, per_peer, group, send_max, quant = dims
    if quant:
        scale_ref, out_ref, out_scale_ref, total_ref, place_ref, seen_ref = refs
    else:
        out_ref, out_scale_ref, total_ref, place_ref, seen_ref = refs
    n = out_ref.shape[0]
    groups, _, width = part_ref.shape
    span = width // group
    total_ref[...] = jnp.zeros_like(total_ref)

    def clear(i, c):
        seen_ref[i] = 0
        return c

    lax.fori_loop(0, n, clear, 0)

    def rank(a, c):
        owner = owner_ref[a]
        before = seen_ref[owner]
        place_ref[a] = owner * send_max + before
        seen_ref[owner] = before + 1
        return c

    lax.fori_loop(0, owner_ref.shape[0], rank, 0)
    lane = lax.broadcasted_iota(jnp.int32, (cv, width), 1)
    column = lax.broadcasted_iota(jnp.int32, (width, width), 0)
    row_lane = lax.broadcasted_iota(jnp.int32, (1, width), 1)

    def body(g, c):
        at = row_lane
        for j in range(group * bps):
            t = g * group + j // bps
            pos = meta_ref[t // per_peer, 0, per_peer + (t % per_peer) * bps + j % bps]
            at = at + jnp.where(row_lane // cv == j, cv * (pos - j), 0)
        hot = jnp.where(column == at, 1.0, 0.0).astype(jnp.bfloat16)
        if quant:
            code = part_ref[g].astype(jnp.int32)
            high = code >> 8
            pieces = [high.astype(jnp.float32), (code - high * 256).astype(jnp.float32)]
            weights = [256.0, 1.0]
        else:
            rest = part_ref[g]
            pieces, weights = [], [1.0, 1.0, 1.0]
            for _ in range(3):
                piece = rest.astype(jnp.bfloat16).astype(jnp.float32)
                pieces.append(piece)
                rest = rest - piece
        placed = 0.0
        for piece, weight in zip(pieces, weights):
            stack = jnp.concatenate(
                [
                    jnp.where((lane >= span * tl) & (lane < span * (tl + 1)), piece, 0.0)
                    for tl in range(group)
                ],
                axis=0,
            ).astype(jnp.bfloat16)
            placed = placed + weight * lax.dot_general(
                stack, hot, NT, preferred_element_type=jnp.float32
            )
        if quant:
            factor = as_column(scale_ref[g], cv)
        for tl in range(group):
            t = g * group + tl
            where = place_ref[meta_ref[t // per_peer, 0, t % per_peer]]
            rows = placed[tl * cv : (tl + 1) * cv]
            if quant:
                rows = rows * factor
            total_ref[where] = total_ref[where] + rows
        return c

    lax.fori_loop(0, groups, body, 0, unroll=2)

    def emit(p, c):
        rows = total_ref[pl.ds(p * send_max, send_max)].reshape(send_max * cv, width)
        out_ref[p], out_scale_ref[p] = coded(rows)
        return c

    lax.fori_loop(0, n, emit, 0, unroll=2)


def gathered_rows(part, scale, meta, owners, n, send_max, group, bps, per_peer):
    groups, cv, width = part.shape
    quant = scale is not None
    args = [meta, owners, part] + ([scale] if quant else [])
    return pl.pallas_call(
        functools.partial(gather_rows_kernel, (cv, bps, per_peer, group, send_max, quant)),
        out_shape=[
            jax.ShapeDtypeStruct((n, send_max * cv, width), jnp.int16),
            jax.ShapeDtypeStruct((n, 1, LANES), jnp.float32),
        ],
        in_specs=[SMEM, SMEM] + [VMEM] * (len(args) - 2),
        out_specs=[VMEM, VMEM],
        scratch_shapes=[
            pltpu.VMEM((n * send_max, cv, width), jnp.float32),
            pltpu.SMEM((owners.shape[0],), jnp.int32),
            pltpu.SMEM((n,), jnp.int32),
        ],
        compiler_params=pltpu.CompilerParams(vmem_limit_bytes=48 << 20),
        name="gathered_rows",
    )(*args)


def per_device(gx, gy, prolong, stiffness, request, col_slot, col_pos, coarse_owner):
    n = gx * gy
    own_aggs, cv, dof = prolong.shape
    slots, bps = col_slot.shape
    per_peer = slots // n
    group = MAXNB // bps
    quant = per_peer == group
    send_max = (2 * own_aggs + n - 1) // n

    meta = jnp.concatenate([request.reshape(n, per_peer), col_pos.reshape(n, per_peer * bps)], axis=1)
    meta = jnp.pad(meta, ((0, 0), (0, LANES - meta.shape[1])))[:, None, :]
    if quant:
        meta_in, part, scale = fused(meta, prolong, stiffness, col_slot, gx, gy, group)
    else:
        (meta_in,) = exchange([meta], gx, gy, 1)
        answer = prolong[meta_in[:, 0, :per_peer].reshape(-1)].reshape(n, per_peer * cv, dof)
        (fetched,) = exchange([answer], gx, gy, 2)
        made = products(fetched.reshape(slots, cv, dof), stiffness, col_slot, group)
        flat = made.reshape(slots // group, cv, group, bps * cv).transpose(0, 2, 1, 3)
        (flat,) = exchange([flat.reshape(n, per_peer * cv, bps * cv)], gx, gy, 3)
        flat = flat.reshape(slots // group, group, cv, bps * cv).transpose(0, 2, 1, 3)
        part, scale = flat.reshape(slots // group, cv, group * bps * cv), None
    code, factor = gathered_rows(
        part, scale, meta_in, coarse_owner[:, 0], n, send_max, group, bps, per_peer
    )
    return delivered(code, factor, cv, gx, gy)


def solution(mesh):
    gx, gy = mesh.shape["gx"], mesh.shape["gy"]
    placed = (
        P(AXES, None, None),
        P(AXES, None, None, None),
        P(AXES),
        P(AXES, None),
        P(AXES, None),
        P(AXES, None),
    )
    return jax.shard_map(
        functools.partial(per_device, gx, gy),
        mesh=mesh,
        in_specs=placed,
        out_specs=P(AXES, None, None),
        check_vma=False,
    )
```

```python
import functools

import jax
import jax.numpy as jnp
from jax import lax
from jax.experimental import pallas as pl
from jax.experimental.pallas import tpu as pltpu
from jax.sharding import PartitionSpec as P

MAXNB = 16
AXES = ("gx", "gy")
LANES = 128
TOP = 32767.0
MESH = pl.DeviceIdType.MESH
HBM = pl.BlockSpec(memory_space=pl.ANY)
VMEM = pl.BlockSpec(memory_space=pltpu.VMEM)
SMEM = pl.BlockSpec(memory_space=pltpu.SMEM)
NT = (((1,), (1,)), ((), ()))


def peer_at(k, gx, gy, mixed):
    n = gx * gy
    x, y = lax.axis_index("gx"), lax.axis_index("gy")
    if gx % 2:
        return lax.rem(x * gy + y + 1 + k, n)
    half = gx // 2
    count = half * gy
    if mixed:
        near, i = lax.rem(k, 2), k // 2
    else:
        near, i = k // count, lax.rem(k, count)
    i = lax.rem(i + near, count)
    side = lax.rem(x // half + 1 + near, 2)
    row = side * half + lax.rem(x + i // gy, half)
    return row * gy + lax.rem(y + i, gy)


def deliver_kernel(dims, code_ref, scale_ref, out_ref, land_ref, land_scale, wide_ref, *sems):
    gx, gy, cv = dims
    code_send, code_recv, scale_send, scale_recv, out_sem = sems
    n, rows, width = code_ref.shape
    take = rows // cv
    me = lax.axis_index("gx") * gy + lax.axis_index("gy")
    barrier = pltpu.get_barrier_semaphore()

    def where(peer):
        return (peer // gy, lax.rem(peer, gy))

    def greet(k, c):
        peer = peer_at(k, gx, gy, True)
        pl.semaphore_signal(barrier, inc=1, device_id=where(peer), device_id_type=MESH)
        return c

    lax.fori_loop(0, n - 1, greet, 0)

    def copies(peer, source):
        return [
            pltpu.make_async_remote_copy(
                src_ref=src.at[peer], dst_ref=dst.at[source],
                send_sem=send.at[peer], recv_sem=recv.at[source],
                device_id=where(peer), device_id_type=MESH,
            )
            for src, dst, send, recv in (
                (scale_ref, land_scale, scale_send, scale_recv),
                (code_ref, land_ref, code_send, code_recv),
            )
        ]

    def out_copy(p):
        at = pl.ds(p * take, take)
        return pltpu.make_async_copy(wide_ref.at[at], out_ref.at[at], out_sem.at[p])

    pl.semaphore_wait(barrier, n - 1)

    def send(k, c):
        for copy in copies(peer_at(k, gx, gy, True), me):
            copy.start()
        return c

    lax.fori_loop(0, n - 1, send, 0)

    def decode(code, scale, p):
        values = code.astype(jnp.int32).astype(jnp.float32) * as_column(scale, rows)
        wide_ref[pl.ds(p * take, take)] = values.reshape(take, cv, width)
        out_copy(p).start()

    decode(code_ref[me], scale_ref[me], me)

    def drain(k, c):
        source = peer_at(k, gx, gy, True)
        for copy in copies(source, source):
            copy.wait()
        decode(land_ref[source], land_scale[source], source)
        return c

    lax.fori_loop(0, n - 1, drain, 0)

    def finish(p, c):
        out_copy(p).wait()
        return c

    lax.fori_loop(0, n, finish, 0)


def delivered(code, scale, cv, gx, gy):
    n, rows, width = code.shape
    sem = pltpu.SemaphoreType.DMA
    out = (n * rows // cv, cv, width)
    return pl.pallas_call(
        functools.partial(deliver_kernel, (gx, gy, cv)),
        out_shape=jax.ShapeDtypeStruct(out, jnp.float32),
        in_specs=[VMEM, VMEM],
        out_specs=HBM,
        scratch_shapes=[
            pltpu.VMEM(code.shape, jnp.int16),
            pltpu.VMEM(scale.shape, jnp.float32),
            pltpu.VMEM(out, jnp.float32),
        ]
        + [sem((n,))] * 5,
        compiler_params=pltpu.CompilerParams(
            collective_id=4, has_side_effects=True, vmem_limit_bytes=40 << 20
        ),
        name="delivered",
    )(code, scale)


def exchange_kernel(gx, gy, count, *refs):
    ins, outs = refs[:count], refs[count : 2 * count]
    send_sem, recv_sem, local_sem = refs[2 * count :]
    n = gx * gy
    me = lax.axis_index("gx") * gy + lax.axis_index("gy")
    barrier = pltpu.get_barrier_semaphore()

    def greet(k, c):
        peer = lax.rem(me + k, n)
        pl.semaphore_signal(barrier, inc=1, device_id=(peer // gy, lax.rem(peer, gy)), device_id_type=MESH)
        return c

    lax.fori_loop(1, n, greet, 0)
    own = [pltpu.make_async_copy(ins[i].at[me], outs[i].at[me], local_sem.at[i]) for i in range(count)]
    for copy in own:
        copy.start()
    pl.semaphore_wait(barrier, n - 1)

    def copies(k, source):
        peer = lax.rem(me + k, n)
        return [
            pltpu.make_async_remote_copy(
                src_ref=ins[i].at[peer],
                dst_ref=outs[i].at[source],
                send_sem=send_sem.at[i, k],
                recv_sem=recv_sem.at[i, k],
                device_id=(peer // gy, lax.rem(peer, gy)),
                device_id_type=MESH,
            )
            for i in range(count)
        ]

    def send(k, c):
        for copy in copies(k, me):
            copy.start()
        return c

    lax.fori_loop(1, n, send, 0)

    def drain(k, c):
        for copy in copies(k, lax.rem(me + n - k, n)):
            copy.wait()
        return c

    lax.fori_loop(1, n, drain, 0)
    for copy in own:
        copy.wait()


def exchange(arrays, gx, gy, number):
    count = len(arrays)
    n = gx * gy
    return pl.pallas_call(
        functools.partial(exchange_kernel, gx, gy, count),
        out_shape=[jax.ShapeDtypeStruct(a.shape, a.dtype) for a in arrays],
        in_specs=[HBM] * count,
        out_specs=[HBM] * count,
        scratch_shapes=[
            pltpu.SemaphoreType.DMA((count, n)),
            pltpu.SemaphoreType.DMA((count, n)),
            pltpu.SemaphoreType.DMA((count,)),
        ],
        compiler_params=pltpu.CompilerParams(collective_id=number, has_side_effects=True),
        name=f"exchange{number}",
    )(*arrays)


def as_row(column):
    rows = column.shape[0]
    shape = (rows, LANES)
    eye = lax.broadcasted_iota(jnp.int32, shape, 0) == lax.broadcasted_iota(jnp.int32, shape, 1)
    return jnp.sum(jnp.where(eye, column, 0.0), axis=0, keepdims=True)


def as_column(row, rows):
    shape = (rows, LANES)
    eye = lax.broadcasted_iota(jnp.int32, shape, 0) == lax.broadcasted_iota(jnp.int32, shape, 1)
    return jnp.sum(jnp.where(eye, row, 0.0), axis=1, keepdims=True)


def coded(values):
    top = jnp.maximum(jnp.max(jnp.abs(values), axis=1, keepdims=True), 1e-30)
    code = jnp.round(values * (TOP / top)).astype(jnp.int32).astype(jnp.int16)
    return code, as_row(top * (1.0 / TOP))


def group_product(dims, grp, slot_ref, wide_ref, cols_ref, mats_of):
    cv, bps, group = dims
    dof = wide_ref.shape[-1]
    span = bps * cv
    lane = lax.broadcasted_iota(jnp.int32, (dof, LANES), 1)
    applied = []
    for tl in range(group):
        for q in range(bps):
            block = wide_ref[slot_ref[grp * group + tl, q]]
            at = (span * tl + cv * q) % LANES
            first = min(cv, LANES - at)
            cols_ref[tl, at : at + first, :] = block[:first]
            if first < cv:
                cols_ref[tl, 0 : cv - first, :] = block[first:]
    for tl in range(group):
        cols = cols_ref[tl].astype(jnp.bfloat16)
        mats = mats_of(tl).reshape(bps * dof, dof)
        prod = lax.dot_general(mats, cols, NT, preferred_element_type=jnp.float32)
        rel = (lane + (LANES * tl - span * tl) % LANES) % LANES
        one = prod[(bps - 1) * dof :]
        for q in range(bps - 2, -1, -1):
            one = jnp.where(rel < cv * (q + 1), prod[q * dof : (q + 1) * dof], one)
        applied.append(one)
    tiles = []
    for j in range(span * group // LANES):
        low, high = LANES * j // span, (LANES * (j + 1) - 1) // span
        tile = applied[high]
        for tl in range(high - 1, low - 1, -1):
            tile = jnp.where(lane < span * (tl + 1) - LANES * j, applied[tl], tile)
        tiles.append(tile)
    whole = jnp.concatenate(tiles, axis=1)
    hi = whole.astype(jnp.bfloat16)
    lo = (whole - hi.astype(jnp.float32)).astype(jnp.bfloat16)
    rows = wide_ref[pl.ds(grp * group, group)].reshape(group * cv, dof).astype(jnp.bfloat16)
    both = jnp.dot(rows, hi, preferred_element_type=jnp.float32) + jnp.dot(
        rows, lo, preferred_element_type=jnp.float32
    )
    wide_lane = lax.broadcasted_iota(jnp.int32, (cv, span * group), 1)
    out = both[(group - 1) * cv :]
    for tl in range(group - 2, -1, -1):
        out = jnp.where(wide_lane < span * (tl + 1), both[tl * cv : (tl + 1) * cv], out)
    return out


def product_kernel(dims, slot_ref, fetched_ref, stiff_ref, out_ref, wide_ref, cols_ref):
    cv, bps, group, per_step = dims
    step = pl.program_id(0)

    @pl.when(step == 0)
    def _():
        wide_ref[...] = fetched_ref[...].astype(jnp.float32)

    def body(k, c):
        out_ref[k] = group_product(
            (cv, bps, group), step * per_step + k, slot_ref, wide_ref, cols_ref,
            lambda tl: stiff_ref[k * group + tl],
        )
        return c

    lax.fori_loop(0, per_step, body, 0)


def products(fetched, stiffness, col_slot, group):
    slots, cv, dof = fetched.shape
    bps = stiffness.shape[1]
    groups = slots // group
    per_step = 4 if groups % 4 == 0 else 1
    width = group * bps * cv
    return pl.pallas_call(
        functools.partial(product_kernel, (cv, bps, group, per_step)),
        grid=(groups // per_step,),
        out_shape=jax.ShapeDtypeStruct((groups, cv, width), jnp.float32),
        in_specs=[
            SMEM,
            pl.BlockSpec((slots, cv, dof), lambda i: (0, 0, 0)),
            pl.BlockSpec((per_step * group, bps, dof, dof), lambda i: (i, 0, 0, 0)),
        ],
        out_specs=pl.BlockSpec((per_step, cv, width), lambda i: (i, 0, 0)),
        scratch_shapes=[
            pltpu.VMEM((slots, cv, dof), jnp.float32),
            pltpu.VMEM((group, LANES, dof), jnp.float32),
        ],
        compiler_params=pltpu.CompilerParams(vmem_limit_bytes=48 << 20),
        name="products",
    )(col_slot, fetched, stiffness)


def fused_kernel(
    dims,
    slot_ref, meta_ref, prolong_ref, stiff_ref,
    meta_out, part_out, scale_out,
    req_ref, stage_ref, fetched_ref, wide_ref, cols_ref, mats_ref, code_ref, factor_ref,
    meta_send, meta_recv, fetch_send, fetch_recv, part_send, part_recv, scale_send, scale_recv,
    mats_sem, own_sem,
):
    gx, gy, cv, bps, group = dims
    n = gx * gy
    me = lax.axis_index("gx") * gy + lax.axis_index("gy")
    barrier = pltpu.get_barrier_semaphore()

    def where(peer):
        return (peer // gy, lax.rem(peer, gy))

    def remote(src, dst, send_sem, recv_sem, peer):
        return pltpu.make_async_remote_copy(
            src_ref=src, dst_ref=dst, send_sem=send_sem, recv_sem=recv_sem,
            device_id=where(peer), device_id_type=MESH,
        )

    def meta_copy(peer, source):
        return remote(
            meta_ref.at[peer], meta_out.at[source], meta_send.at[peer], meta_recv.at[source], peer
        )

    def fetch_copy(peer, source):
        return remote(
            stage_ref.at[pl.ds(peer * group, group)],
            fetched_ref.at[pl.ds(source * group, group)],
            fetch_send.at[peer], fetch_recv.at[source], peer,
        )

    def part_copies(peer, source):
        return (
            remote(code_ref.at[peer], part_out.at[source], part_send.at[peer], part_recv.at[source], peer),
            remote(
                factor_ref.at[peer], scale_out.at[source], scale_send.at[peer], scale_recv.at[source], peer
            ),
        )

    def mats_copy(peer):
        return pltpu.make_async_copy(
            stiff_ref.at[pl.ds(peer * group, group)],
            mats_ref.at[pl.ds(peer * group, group)],
            mats_sem.at[peer],
        )

    def greet(k, c):
        pl.semaphore_signal(barrier, inc=1, device_id=where(lax.rem(me + k, n)), device_id_type=MESH)
        return c

    lax.fori_loop(1, n, greet, 0)
    own_meta = pltpu.make_async_copy(meta_ref.at[me], meta_out.at[me], own_sem.at[0])
    own_meta.start()

    def load(k, c):
        mats_copy(peer_at(k, gx, gy, False)).start()
        return c

    lax.fori_loop(0, n, load, 0)
    pl.semaphore_wait(barrier, n - 1)

    def ask(k, c):
        meta_copy(peer_at(k, gx, gy, True), me).start()
        return c

    lax.fori_loop(0, n - 1, ask, 0)
    own_meta.wait()

    def asked(k, c):
        source = peer_at(k, gx, gy, True)
        meta_copy(source, source).wait()
        return c

    lax.fori_loop(0, n - 1, asked, 0)
    to_scalars = pltpu.make_async_copy(meta_out, req_ref, own_sem.at[1])
    to_scalars.start()
    to_scalars.wait()

    def fill(k, c):
        peer = peer_at(k, gx, gy, True)
        for j in range(group):
            stage_ref[peer * group + j] = prolong_ref[req_ref[peer, 0, j]]
        return c

    lax.fori_loop(0, n, fill, 0)

    def answer(k, c):
        fetch_copy(peer_at(k, gx, gy, True), me).start()
        return c

    lax.fori_loop(0, n - 1, answer, 0)
    for j in range(group):
        wide_ref[me * group + j] = stage_ref[me * group + j].astype(jnp.float32)

    def take(k, c):
        source = peer_at(k, gx, gy, True)
        fetch_copy(source, source).wait()
        for j in range(group):
            wide_ref[source * group + j] = fetched_ref[source * group + j].astype(jnp.float32)
        return c

    lax.fori_loop(0, n - 1, take, 0)
    wide_step = 2 if n % 2 == 0 else 1

    def work(i, c):
        for u in range(wide_step):
            mats_copy(peer_at(i * wide_step + u, gx, gy, False)).wait()
        for u in range(wide_step):
            peer = peer_at(i * wide_step + u, gx, gy, False)
            out = group_product(
                (cv, bps, group), peer, slot_ref, wide_ref, cols_ref.at[u],
                lambda tl: mats_ref[peer * group + tl],
            )
            code_ref[peer], factor_ref[peer] = coded(out)

        @pl.when(i > 0)
        def _():
            for u in range(wide_step):
                for copy in part_copies(peer_at((i - 1) * wide_step + u, gx, gy, False), me):
                    copy.start()

        return c

    lax.fori_loop(0, n // wide_step, work, 0)
    for k in range(n - wide_step, n - 1):
        for copy in part_copies(peer_at(k, gx, gy, False), me):
            copy.start()
    own = (
        pltpu.make_async_copy(code_ref.at[me], part_out.at[me], own_sem.at[2]),
        pltpu.make_async_copy(factor_ref.at[me], scale_out.at[me], own_sem.at[3]),
    )
    for copy in own:
        copy.start()

    def drain(k, c):
        source = peer_at(k, gx, gy, False)
        for copy in part_copies(source, source):
            copy.wait()
        return c

    lax.fori_loop(0, n - 1, drain, 0)
    for copy in own:
        copy.wait()


def fused(meta, prolong, stiffness, col_slot, gx, gy, group):
    slots, bps, dof, _ = stiffness.shape
    cv = prolong.shape[1]
    n = gx * gy
    width = group * bps * cv
    sem = pltpu.SemaphoreType.DMA
    return pl.pallas_call(
        functools.partial(fused_kernel, (gx, gy, cv, bps, group)),
        out_shape=[
            jax.ShapeDtypeStruct(meta.shape, jnp.int32),
            jax.ShapeDtypeStruct((n, cv, width), jnp.int16),
            jax.ShapeDtypeStruct((n, 1, LANES), jnp.float32),
        ],
        in_specs=[SMEM, VMEM, VMEM, HBM],
        out_specs=[VMEM, VMEM, VMEM],
        scratch_shapes=[
            pltpu.SMEM(meta.shape, jnp.int32),
            pltpu.VMEM((slots, cv, dof), jnp.bfloat16),
            pltpu.VMEM((slots, cv, dof), jnp.bfloat16),
            pltpu.VMEM((slots, cv, dof), jnp.float32),
            pltpu.VMEM((2, group, LANES, dof), jnp.float32),
            pltpu.VMEM((slots, bps, dof, dof), jnp.bfloat16),
            pltpu.VMEM((n, cv, width), jnp.int16),
            pltpu.VMEM((n, 1, LANES), jnp.float32),
        ]
        + [sem((n,))] * 9
        + [sem((4,))],
        compiler_params=pltpu.CompilerParams(
            collective_id=1, has_side_effects=True, vmem_limit_bytes=56 << 20
        ),
        name="fused",
    )(col_slot, meta, prolong, stiffness)


def gather_rows_kernel(dims, meta_ref, owner_ref, part_ref, *refs):
    cv, bps, per_peer, group, send_max, quant = dims
    if quant:
        scale_ref, out_ref, out_scale_ref, total_ref, place_ref, seen_ref = refs
    else:
        out_ref, out_scale_ref, total_ref, place_ref, seen_ref = refs
    n = out_ref.shape[0]
    groups, _, width = part_ref.shape
    span = width // group
    total_ref[...] = jnp.zeros_like(total_ref)

    def clear(i, c):
        seen_ref[i] = 0
        return c

    lax.fori_loop(0, n, clear, 0)

    def rank(a, c):
        owner = owner_ref[a]
        before = seen_ref[owner]
        place_ref[a] = owner * send_max + before
        seen_ref[owner] = before + 1
        return c

    lax.fori_loop(0, owner_ref.shape[0], rank, 0)
    lane = lax.broadcasted_iota(jnp.int32, (cv, width), 1)
    column = lax.broadcasted_iota(jnp.int32, (width, width), 0)
    row_lane = lax.broadcasted_iota(jnp.int32, (1, width), 1)

    def body(g, c):
        at = row_lane
        for j in range(group * bps):
            t = g * group + j // bps
            pos = meta_ref[t // per_peer, 0, per_peer + (t % per_peer) * bps + j % bps]
            at = at + jnp.where(row_lane // cv == j, cv * (pos - j), 0)
        hot = jnp.where(column == at, 1.0, 0.0).astype(jnp.bfloat16)
        if quant:
            code = part_ref[g].astype(jnp.int32)
            high = code >> 8
            pieces = [high.astype(jnp.float32), (code - high * 256).astype(jnp.float32)]
            weights = [256.0, 1.0]
        else:
            rest = part_ref[g]
            pieces, weights = [], [1.0, 1.0, 1.0]
            for _ in range(3):
                piece = rest.astype(jnp.bfloat16).astype(jnp.float32)
                pieces.append(piece)
                rest = rest - piece
        placed = 0.0
        for piece, weight in zip(pieces, weights):
            stack = jnp.concatenate(
                [
                    jnp.where((lane >= span * tl) & (lane < span * (tl + 1)), piece, 0.0)
                    for tl in range(group)
                ],
                axis=0,
            ).astype(jnp.bfloat16)
            placed = placed + weight * lax.dot_general(
                stack, hot, NT, preferred_element_type=jnp.float32
            )
        if quant:
            factor = as_column(scale_ref[g], cv)
        for tl in range(group):
            t = g * group + tl
            where = place_ref[meta_ref[t // per_peer, 0, t % per_peer]]
            rows = placed[tl * cv : (tl + 1) * cv]
            if quant:
                rows = rows * factor
            total_ref[where] = total_ref[where] + rows
        return c

    lax.fori_loop(0, groups, body, 0, unroll=4)

    def emit(p, c):
        rows = total_ref[pl.ds(p * send_max, send_max)].reshape(send_max * cv, width)
        out_ref[p], out_scale_ref[p] = coded(rows)
        return c

    lax.fori_loop(0, n, emit, 0, unroll=4)


def gathered_rows(part, scale, meta, owners, n, send_max, group, bps, per_peer):
    groups, cv, width = part.shape
    quant = scale is not None
    args = [meta, owners, part] + ([scale] if quant else [])
    return pl.pallas_call(
        functools.partial(gather_rows_kernel, (cv, bps, per_peer, group, send_max, quant)),
        out_shape=[
            jax.ShapeDtypeStruct((n, send_max * cv, width), jnp.int16),
            jax.ShapeDtypeStruct((n, 1, LANES), jnp.float32),
        ],
        in_specs=[SMEM, SMEM] + [VMEM] * (len(args) - 2),
        out_specs=[VMEM, VMEM],
        scratch_shapes=[
            pltpu.VMEM((n * send_max, cv, width), jnp.float32),
            pltpu.SMEM((owners.shape[0],), jnp.int32),
            pltpu.SMEM((n,), jnp.int32),
        ],
        compiler_params=pltpu.CompilerParams(vmem_limit_bytes=48 << 20),
        name="gathered_rows",
    )(*args)


def per_device(gx, gy, prolong, stiffness, request, col_slot, col_pos, coarse_owner):
    n = gx * gy
    own_aggs, cv, dof = prolong.shape
    slots, bps = col_slot.shape
    per_peer = slots // n
    group = MAXNB // bps
    quant = per_peer == group
    send_max = (2 * own_aggs + n - 1) // n

    meta = jnp.concatenate([request.reshape(n, per_peer), col_pos.reshape(n, per_peer * bps)], axis=1)
    meta = jnp.pad(meta, ((0, 0), (0, LANES - meta.shape[1])))[:, None, :]
    if quant:
        meta_in, part, scale = fused(meta, prolong, stiffness, col_slot, gx, gy, group)
    else:
        (meta_in,) = exchange([meta], gx, gy, 1)
        answer = prolong[meta_in[:, 0, :per_peer].reshape(-1)].reshape(n, per_peer * cv, dof)
        (fetched,) = exchange([answer], gx, gy, 2)
        made = products(fetched.reshape(slots, cv, dof), stiffness, col_slot, group)
        flat = made.reshape(slots // group, cv, group, bps * cv).transpose(0, 2, 1, 3)
        (flat,) = exchange([flat.reshape(n, per_peer * cv, bps * cv)], gx, gy, 3)
        flat = flat.reshape(slots // group, group, cv, bps * cv).transpose(0, 2, 1, 3)
        part, scale = flat.reshape(slots // group, cv, group * bps * cv), None
    code, factor = gathered_rows(
        part, scale, meta_in, coarse_owner[:, 0], n, send_max, group, bps, per_peer
    )
    return delivered(code, factor, cv, gx, gy)


def solution(mesh):
    gx, gy = mesh.shape["gx"], mesh.shape["gy"]
    placed = (
        P(AXES, None, None),
        P(AXES, None, None, None),
        P(AXES),
        P(AXES, None),
        P(AXES, None),
        P(AXES, None),
    )
    return jax.shard_map(
        functools.partial(per_device, gx, gy),
        mesh=mesh,
        in_specs=placed,
        out_specs=P(AXES, None, None),
        check_vma=False,
    )
```
